32 devices in a mesh: section: 2 (over x), dp: 16 (over z, y, core).
Axes of the slice: x: 2, y: 2, z: 4, core: 2. Of those that a mesh axis runs over, the one named last changes fastest.
Arguments:
- grads: bfloat16 [32, 524288], P(('section', 'dp')), parts along dimension 0, may hold values from -6 to 6
- master: float32 [32, 32768], P(('section', 'dp')), parts along dimension 0, may hold values from -30 to 30
- first_moment: float32 [32, 32768], P(('section', 'dp')), parts along dimension 0, may hold values from -0.6 to 0.6
- second_moment: float32 [32, 32768], P(('section', 'dp')), parts along dimension 0, may hold values from 0.005 to 0.05
- perm: int32 [32], P('section'), parts along dimension 0, may hold values from 0 to 15, each once
- bounds: int32 [34], P('section'), parts along dimension 0, may hold values from 0 to 524288, as said below
Outputs:
- new_weights: bfloat16 [1048576], P('section'), parts along dimension 0
- new_master: float32 [32, 32768], P(('section', 'dp')), parts along dimension 0
- new_first: float32 [32, 32768], P(('section', 'dp')), parts along dimension 0
- new_second: float32 [32, 32768], P(('section', 'dp')), parts along dimension 0
- step_taken: float32 [32, 32768], P(('section', 'dp')), parts along dimension 0
The draws below stay inside these ranges and needn't reach their ends.
There are 2 independent parts, one for each index of `section`. The reference program is written for one: setup_inputs(seed, part) draws one part's arguments, and reference() takes and returns one part's arrays. A program takes and returns all parts, laid end to end along the dimension named above; each array names one. Nothing has to cross between parts.
Inputs may be any that keep to these rules, and one draw needn't show every extreme that they name: `perm`: each device index appears exactly once. `bounds`: strictly increasing multiples of 128, the first 0 and the last 524288.
All inputs are finite; a program needn't handle non-finite values.
Results may differ from the reference program's by a relative error of at most 0.0004.
Values may be sent and summed in bfloat16 or wider, within the bound.
No kernel may reach another device: no remote copies, remote signals or barrier semaphores. Data moves between devices by JAX's collectives and lax.ppermute only.
A program may use at most 128 MiB of HBM per device.

```python
import math
import jax
import jax.numpy as jnp
from jax import lax

SHARD = 32768
TENSORS = 16
REPLICAS = 16
TOTAL = 524288


def draw_master(key, part):
    noise_key, scale_key = jax.random.split(jax.random.fold_in(key, 11))
    row_pos = jnp.arange(REPLICAS, dtype=jnp.float32)[:, None] / max(REPLICAS - 1, 1)
    base = jnp.clip(jax.random.normal(noise_key, (REPLICAS, SHARD), jnp.float32), -4.0, 4.0)
    spread = math.log(3.0)
    block_scale = jnp.exp(spread * jax.random.uniform(scale_key, (REPLICAS, SHARD // 128, 1), jnp.float32))
    block_scale = jnp.broadcast_to(block_scale, (REPLICAS, SHARD // 128, 128)).reshape(REPLICAS, SHARD)
    rising = jnp.exp(math.log(3.0) * row_pos)
    return (0.25 * base * block_scale * rising).astype(jnp.float32)


def draw_bounds(key, part):
    units = TOTAL // 128
    shuffled = jax.random.permutation(jax.random.fold_in(key, 23), units - 1) + 1
    cuts = jnp.sort(shuffled[:TENSORS - 1]).astype(jnp.int32) * 128
    return jnp.concatenate([jnp.zeros((1,), jnp.int32), cuts, jnp.full((1,), TOTAL, jnp.int32)]).astype(jnp.int32)


def with_spikes(entries, stream_key, source, target, shards_of, factor):
    owner, partner = [(jnp.arange(entries.shape[axis_at]) // (entries.shape[axis_at] // shards_of)).reshape([-1 if axis == axis_at else 1 for axis in range(entries.ndim)]) for axis_at in (source, target)]
    chosen = jax.random.permutation(stream_key, shards_of)[partner]
    strong = (owner == chosen) | (owner == (partner + shards_of // 2) % shards_of)
    return jnp.where(strong, factor * entries, entries)


def level_of(own_key, dims, cuts, least, largest):
    factor_of, own = 1.0, jax.random.fold_in(own_key, 6)
    for dim, blocks in cuts:
        steps = jnp.exp(jax.random.uniform(jax.random.fold_in(own, dim), (blocks,), jnp.float32, least / len(cuts), largest / len(cuts)))
        factor_of = factor_of * jnp.repeat(steps, dims[dim] // blocks).reshape([-1 if axis == dim else 1 for axis in range(len(dims))])
    return factor_of


def centred(rng, shape, scale, most, shards=(), held_as=jnp.bfloat16):
    array = jax.random.normal(rng, shape, jnp.float32) * scale
    if len(shards) > 0:
        array = level_of(rng, shape, shards, -0.22, 0.18) * array
    return jnp.clip(array, min=-most, max=most).astype(held_as)


def bell_draw_with(own_key, dims, scale, bound, cuts, heavy, held_as=jnp.bfloat16):
    entries = scale * jax.random.normal(own_key, dims, jnp.float32)
    if cuts:
        entries = entries * level_of(own_key, dims, cuts, -0.22, 0.18)
    return jnp.clip(with_spikes(entries, jax.random.fold_in(own_key, 3), *heavy), -bound, bound).astype(held_as)


def setup_inputs(seed: int = 0, part: int = 0) -> dict:
    keys = jax.random.split(jax.random.key(seed), 7)
    part_splits = jax.random.split(jax.random.fold_in(keys[6], part), 7)
    grads = bell_draw_with(part_splits[0], (REPLICAS, TOTAL), 1.0, 6.0, ((0, 16),), (0, 1, 16, 2.0))
    master = draw_master(jax.random.fold_in(jax.random.fold_in(keys[6], part), 71), part)
    first_moment = centred(part_splits[2], (REPLICAS, SHARD), 0.1, 0.6, ((0, 16),), jnp.float32)
    second_moment = jnp.clip(jnp.exp(math.log(0.05) - 2.3025851 * jax.random.uniform(part_splits[3], (REPLICAS, SHARD), jnp.float32) ** level_of(part_splits[3], (REPLICAS, SHARD), ((0, 16),), -0.2, 0.2)), 0.005, 0.05)
    perm = jax.random.permutation(part_splits[4], REPLICAS).astype(jnp.int32)
    bounds = draw_bounds(jax.random.fold_in(jax.random.fold_in(keys[6], part), 71), part)
    return dict(grads=grads, master=master, first_moment=first_moment, second_moment=second_moment, perm=perm, bounds=bounds)


beta_first = 0.9
beta_second = 0.999
first_fix = 1.0 - 0.9 ** 10
second_fix = 1.0 - 0.999 ** 10
adam_eps = 1e-06
norm_eps = 1e-06
decay_rate = 0.01
learn_rate = 0.01

def reference(grads, master, first_moment, second_moment, perm, bounds):
    mean_grad = lax.optimization_barrier(jnp.sum(grads.astype(jnp.float32), axis=0)) / REPLICAS
    own_grad = jnp.take(mean_grad.reshape(REPLICAS, SHARD), perm, axis=0)
    new_first = beta_first * first_moment + (1.0 - beta_first) * own_grad
    new_second = beta_second * second_moment + (1.0 - beta_second) * own_grad * own_grad
    direction = new_first / first_fix / (jnp.sqrt(new_second / second_fix) + adam_eps) + decay_rate * master
    positions = perm.astype(jnp.int32)[:, None] * SHARD + jnp.arange(SHARD, dtype=jnp.int32)[None, :]
    tensor_ids = lax.optimization_barrier(jnp.sum((positions[:, :, None] >= bounds[None, None, 1:TENSORS]).astype(jnp.int32), axis=-1)).reshape(-1)
    weight_sq = jax.ops.segment_sum((master * master).reshape(-1), tensor_ids, TENSORS)
    update_sq = jax.ops.segment_sum((direction * direction).reshape(-1), tensor_ids, TENSORS)
    trust_ratio = jnp.sqrt(weight_sq) / (jnp.sqrt(update_sq) + norm_eps)
    step_taken = jnp.take(trust_ratio, tensor_ids).reshape(REPLICAS, SHARD) * direction
    new_master = master - learn_rate * step_taken
    inverse = jnp.argsort(perm)
    new_weights = jnp.take(new_master.astype(jnp.bfloat16), inverse, axis=0).reshape(-1)
    return (new_weights, new_master, new_first, new_second, step_taken)
```

```python
import functools

import jax
import jax.numpy as jnp
from jax import lax
from jax.experimental import pallas as pl
from jax.experimental.pallas import tpu as pltpu
from jax.sharding import PartitionSpec as P

beta_first = 0.9
beta_second = 0.999
first_fix = 1.0 - 0.9**10
second_fix = 1.0 - 0.999**10
adam_eps = 1e-06
norm_eps = 1e-06
decay_rate = 0.01
learn_rate = 0.01

LANES = 128
WIRE_SCALE = 1024.0


ANY = pl.BlockSpec(memory_space=pl.ANY)
SMEM = pl.BlockSpec(memory_space=pltpu.SMEM)
VMEM = pl.BlockSpec(memory_space=pltpu.VMEM)


def take_blocks_kernel(index_ref, grads_ref, out_ref, rows_ref, sems):
    count, shard_rows, _ = out_ref.shape
    shard_len = shard_rows * LANES

    def fetch(k):
        start = pl.multiple_of(index_ref[k] * shard_len, shard_len)
        return pltpu.make_async_copy(
            grads_ref.at[:, pl.ds(start, shard_len)], rows_ref.at[k], sems.at[k]
        )

    for k in range(count):
        fetch(k).start()
    for k in range(count):
        fetch(k).wait()
        out_ref[k] = rows_ref[k].reshape(shard_rows, LANES)


def take_blocks(grads, index, shard_len):
    count = index.shape[0]
    return pl.pallas_call(
        take_blocks_kernel,
        out_shape=jax.ShapeDtypeStruct((count, shard_len // LANES, LANES), grads.dtype),
        in_specs=[SMEM, ANY],
        out_specs=VMEM,
        scratch_shapes=[
            pltpu.VMEM((count, 1, shard_len), grads.dtype),
            pltpu.SemaphoreType.DMA((count,)),
        ],
        name="take_blocks",
    )(index, grads)


def member_rows(block_ref, bounds_ref, t, shape):
    rows = lax.broadcasted_iota(jnp.int32, shape, 0)
    first = block_ref[0] * shape[0]
    low = bounds_ref[t] // LANES - first
    high = bounds_ref[t + 1] // LANES - first
    return (rows >= low) & (rows < high)


def sums_kernel(block_ref, bounds_ref, master_ref, direction_ref, out_ref):
    tensors = bounds_ref.shape[0] - 1
    master = master_ref[...]
    direction = direction_ref[...]
    weight_sq = master * master
    update_sq = direction * direction
    for t in range(tensors):
        member = member_rows(block_ref, bounds_ref, t, master.shape)
        out_ref[0, t, :] = jnp.sum(jnp.where(member, weight_sq, 0.0), axis=0)
        out_ref[1, t, :] = jnp.sum(jnp.where(member, update_sq, 0.0), axis=0)


def tensor_sums(block, bounds, master, direction):
    tensors = bounds.shape[0] - 1
    return pl.pallas_call(
        sums_kernel,
        out_shape=jax.ShapeDtypeStruct((2, tensors, LANES), jnp.float32),
        in_specs=[SMEM, SMEM, VMEM, VMEM],
        out_specs=VMEM,
        name="tensor_sums",
    )(block, bounds, master, direction)


def finish_kernel(
    block_ref, bounds_ref, sums_ref, master_ref, direction_ref, step_ref, new_ref, weights_ref
):
    tensors = bounds_ref.shape[0] - 1
    sums = jnp.sum(sums_ref[...], axis=0)
    norms = jnp.sqrt(jnp.sum(sums, axis=-1, keepdims=True))
    ratios = norms[0] / (norms[1] + norm_eps)
    master = master_ref[...]
    ratio = jnp.zeros(master.shape, jnp.float32)
    for t in range(tensors):
        member = member_rows(block_ref, bounds_ref, t, master.shape)
        ratio = jnp.where(member, ratios[t : t + 1, :], ratio)
    step = ratio * direction_ref[...]
    new = master - learn_rate * step
    step_ref[...] = step
    new_ref[...] = new
    weights_ref[...] = new.astype(jnp.bfloat16)


def finish(block, bounds, sums, master, direction):
    like = jax.ShapeDtypeStruct(master.shape, jnp.float32)
    return pl.pallas_call(
        finish_kernel,
        out_shape=(like, like, jax.ShapeDtypeStruct(master.shape, jnp.bfloat16)),
        in_specs=[SMEM, SMEM, VMEM, VMEM, VMEM],
        out_specs=(VMEM, VMEM, VMEM),
        name="finish",
    )(block, bounds, sums, master, direction)


def place_kernel(index_ref, *refs):
    pieces, out_ref, sems = refs[:-2], refs[-2], refs[-1]

    def put(k):
        return pltpu.make_async_copy(pieces[k], out_ref.at[index_ref[k]], sems.at[k])

    for k in range(len(pieces)):
        put(k).start()
    for k in range(len(pieces)):
        put(k).wait()


def place(pieces, index):
    count = len(pieces)
    return pl.pallas_call(
        place_kernel,
        out_shape=jax.ShapeDtypeStruct((count, *pieces[0].shape), pieces[0].dtype),
        in_specs=[SMEM] + [ANY] * count,
        out_specs=ANY,
        scratch_shapes=[pltpu.SemaphoreType.DMA((count,))],
        name="place",
    )(index, *pieces)


def per_device(grads, master, first_moment, second_moment, perm, bounds):
    count = lax.axis_size("dp")
    if count & (count - 1):
        raise ValueError("unsupported dp size")
    half = count // 2
    shard_len = master.shape[1]
    shard_rows = shard_len // LANES
    me = lax.axis_index("dp")

    def swap(value, offset):
        return lax.ppermute(value, "dp", [(i, i ^ offset) for i in range(count)])

    others = 2 * jnp.arange(half, dtype=jnp.int32)
    given = take_blocks(grads, perm[(me ^ 1) ^ others], shard_len)
    kept = take_blocks(grads, perm[me ^ others], shard_len)
    taken = swap(given, 1)
    total = kept[0].astype(jnp.float32) + taken[0].astype(jnp.float32)
    arrived = []
    for k in range(1, half):
        pair = kept[k].astype(jnp.float32) + taken[k].astype(jnp.float32)
        arrived.append(swap((pair * WIRE_SCALE).astype(jnp.float16), 2 * k))
    for piece in arrived:
        total = total + piece.astype(jnp.float32) * (1.0 / WIRE_SCALE)
    own_grad = total / count

    master = master.reshape(shard_rows, LANES)
    first_moment = first_moment.reshape(shard_rows, LANES)
    second_moment = second_moment.reshape(shard_rows, LANES)
    new_first = beta_first * first_moment + (1.0 - beta_first) * own_grad
    new_second = beta_second * second_moment + (1.0 - beta_second) * own_grad * own_grad
    direction = (
        new_first / first_fix / (jnp.sqrt(new_second / second_fix) + adam_eps) + decay_rate * master
    )
    block = perm[me][None]
    sums = tensor_sums(block, bounds, master, direction)
    every = lax.all_to_all(
        jnp.broadcast_to(sums[None], (count, *sums.shape)), "dp", 0, 0, tiled=True
    )
    step_taken, new_master, weights = finish(block, bounds, every, master, direction)

    pieces = {0: weights}
    offset = half
    while offset:
        pieces |= {k ^ offset: swap(piece, offset) for k, piece in pieces.items()}
        offset //= 2
    order = jnp.arange(count, dtype=jnp.int32)
    new_weights = place([pieces[k] for k in range(count)], perm[me ^ order])

    def row(value):
        return value.reshape(1, shard_len)

    return (
        new_weights.reshape(-1),
        row(new_master),
        row(new_first),
        row(new_second),
        row(step_taken),
    )


def solution(mesh):
    rows = P(("section", "dp"), None)
    return jax.shard_map(
        per_device,
        mesh=mesh,
        in_specs=(rows, rows, rows, rows, P("section"), P("section")),
        out_specs=(P("section"), rows, rows, rows, rows),
        check_vma=False,
    )
```

```python
import functools
import math

import jax
import jax.numpy as jnp
from jax import lax
from jax.experimental import pallas as pl
from jax.experimental.pallas import tpu as pltpu
from jax.sharding import PartitionSpec as P

beta_first = 0.9
beta_second = 0.999
first_fix = 1.0 - 0.9**10
second_fix = 1.0 - 0.999**10
adam_eps = 1e-06
norm_eps = 1e-06
decay_rate = 0.01
learn_rate = 0.01

LANES = 128
WIRE_SCALE = 1024.0


ANY = pl.BlockSpec(memory_space=pl.ANY)
SMEM = pl.BlockSpec(memory_space=pltpu.SMEM)
VMEM = pl.BlockSpec(memory_space=pltpu.VMEM)


NEAR_BYTES = 1 << 20


def fits(count, shape, dtype):
    return count * math.prod(shape) * jnp.dtype(dtype).itemsize <= NEAR_BYTES


def near(value):
    return pltpu.with_memory_space_constraint(value, pltpu.VMEM)


def output(shape, dtype):
    kind = pltpu.VMEM if fits(1, shape, dtype) else jax.ShapeDtypeStruct
    return kind(shape, dtype)


def take_blocks_kernel(flip, perm_ref, grads_ref, out_ref, rows_ref, sems):
    count, shard_rows, _ = out_ref.shape
    shard_len = shard_rows * LANES
    target = lax.axis_index("dp") ^ flip

    def fetch(k):
        start = pl.multiple_of(perm_ref[target ^ (2 * k)] * shard_len, shard_len)
        return pltpu.make_async_copy(
            grads_ref.at[:, pl.ds(start, shard_len)], rows_ref.at[k], sems.at[k]
        )

    for k in range(count):
        fetch(k).start()
    for k in range(count):
        fetch(k).wait()
        out_ref[k] = rows_ref[k].reshape(shard_rows, LANES)


def take_blocks(grads, perm, shard_len, flip):
    count = perm.shape[0] // 2
    return pl.pallas_call(
        functools.partial(take_blocks_kernel, flip),
        out_shape=output((count, shard_len // LANES, LANES), grads.dtype),
        in_specs=[SMEM, ANY],
        out_specs=VMEM,
        scratch_shapes=[
            pltpu.VMEM((count, 1, shard_len), grads.dtype),
            pltpu.SemaphoreType.DMA((count,)),
        ],
        name="take_blocks",
    )(perm, grads)


def block_start(perm_ref, shard_rows):
    return perm_ref[lax.axis_index("dp")] * shard_rows


def sums_kernel(perm_ref, bounds_ref, master_ref, direction_ref, out_ref):
    tensors = bounds_ref.shape[0] - 1
    shard_rows = master_ref.shape[0]
    first = block_start(perm_ref, shard_rows)
    shape = (tensors, shard_rows)
    tensor = lax.broadcasted_iota(jnp.int32, shape, 0)
    row = lax.broadcasted_iota(jnp.int32, shape, 1)
    low = jnp.zeros(shape, jnp.int32)
    high = jnp.zeros(shape, jnp.int32)
    for t in range(tensors):
        low = jnp.where(tensor == t, bounds_ref[t] // LANES - first, low)
        high = jnp.where(tensor == t, bounds_ref[t + 1] // LANES - first, high)
    member = ((row >= low) & (row < high)).astype(jnp.float32)

    def per_tensor(value):
        sums = jnp.dot(
            member,
            value * value,
            precision=lax.Precision.HIGHEST,
            preferred_element_type=jnp.float32,
        )
        return jnp.sum(sums, axis=1, keepdims=True)

    weight_sq = per_tensor(master_ref[...])
    update_sq = per_tensor(direction_ref[...])
    lane = lax.broadcasted_iota(jnp.int32, (tensors, LANES), 1)
    packed = jnp.where(lane == 0, weight_sq, jnp.where(lane == 1, update_sq, 0.0))
    out_ref[...] = jnp.broadcast_to(packed[None], out_ref.shape)


def tensor_sums(perm, bounds, master, direction, copies):
    tensors = bounds.shape[0] - 1
    return pl.pallas_call(
        sums_kernel,
        out_shape=output((copies, tensors, LANES), jnp.float32),
        in_specs=[SMEM, SMEM, VMEM, VMEM],
        out_specs=VMEM,
        name="tensor_sums",
    )(perm, bounds, near(master), near(direction))


def finish_kernel(
    perm_ref, bounds_ref, sums_ref, master_ref, direction_ref, step_ref, new_ref, weights_ref
):
    tensors = bounds_ref.shape[0] - 1
    shape = master_ref.shape
    norms = jnp.sqrt(jnp.sum(sums_ref[...], axis=0))
    ratios = norms[:, 0:1] / (norms[:, 1:2] + norm_eps)
    row = lax.broadcasted_iota(jnp.int32, shape, 0) + block_start(perm_ref, shape[0])
    ratio = jnp.broadcast_to(ratios[0:1], shape)
    for t in range(1, tensors):
        ratio = jnp.where(row >= bounds_ref[t] // LANES, ratios[t : t + 1], ratio)
    step = ratio * direction_ref[...]
    new = master_ref[...] - learn_rate * step
    step_ref[...] = step
    new_ref[...] = new
    weights_ref[...] = new.astype(jnp.bfloat16)


def finish(perm, bounds, sums, master, direction):
    return pl.pallas_call(
        finish_kernel,
        out_shape=(
            pltpu.VMEM(master.shape, jnp.float32),
            pltpu.VMEM(master.shape, jnp.float32),
            pltpu.VMEM(master.shape, jnp.bfloat16),
        ),
        in_specs=[SMEM, SMEM, VMEM, VMEM, VMEM],
        out_specs=(VMEM, VMEM, VMEM),
        name="finish",
    )(perm, bounds, near(sums), near(master), near(direction))


def place_kernel(count, perm_ref, *refs):
    pieces, rows = refs[:count], refs[count:-1]
    sems = refs[-1]
    kept, (out_ref, *rows_out) = rows[: len(rows) // 2], rows[len(rows) // 2 :]
    me = lax.axis_index("dp")
    copies = [
        pltpu.make_async_copy(pieces[k], out_ref.at[perm_ref[me ^ k]], sems.at[k])
        for k in range(count)
    ]
    for k, (source, target) in enumerate(zip(kept, rows_out)):
        copies.append(pltpu.make_async_copy(source, target, sems.at[count + k]))
    for copy in copies:
        copy.start()
    for copy in copies:
        copy.wait()


def place(perm, pieces, rows):
    count = len(pieces)
    like = pieces[0]
    close = fits(count, like.shape, like.dtype)
    return pl.pallas_call(
        functools.partial(place_kernel, count),
        out_shape=(
            jax.ShapeDtypeStruct((count, *like.shape), like.dtype),
            *(jax.ShapeDtypeStruct(row.shape, row.dtype) for row in rows),
        ),
        in_specs=[SMEM] + [VMEM if close else ANY] * count + [VMEM] * len(rows),
        out_specs=(ANY,) * (1 + len(rows)),
        scratch_shapes=[pltpu.SemaphoreType.DMA((count + len(rows),))],
        name="place",
    )(perm, *(map(near, pieces) if close else pieces), *map(near, rows))


def per_device(grads, master, first_moment, second_moment, perm, bounds):
    count = lax.axis_size("dp")
    if count & (count - 1):
        raise ValueError("unsupported dp size")
    half = count // 2
    shard_len = master.shape[1]
    shard_rows = shard_len // LANES

    def swap(value, offset):
        return lax.ppermute(value, "dp", [(i, i ^ offset) for i in range(count)])

    given = take_blocks(grads, perm, shard_len, 1)
    kept = take_blocks(grads, perm, shard_len, 0)
    taken = swap(given, 1)
    total = kept[0].astype(jnp.float32) + taken[0].astype(jnp.float32)
    arrived = []
    for k in range(1, half):
        pair = kept[k].astype(jnp.float32) + taken[k].astype(jnp.float32)
        arrived.append(swap((pair * WIRE_SCALE).astype(jnp.float16), 2 * k))
    for piece in arrived:
        total = total + piece.astype(jnp.float32) * (1.0 / WIRE_SCALE)
    own_grad = total / count

    master = master.reshape(shard_rows, LANES)
    first_moment = first_moment.reshape(shard_rows, LANES)
    second_moment = second_moment.reshape(shard_rows, LANES)
    new_first = beta_first * first_moment + (1.0 - beta_first) * own_grad
    new_second = beta_second * second_moment + (1.0 - beta_second) * own_grad * own_grad
    direction = (
        new_first / first_fix / (jnp.sqrt(new_second / second_fix) + adam_eps) + decay_rate * master
    )
    sums = tensor_sums(perm, bounds, master, direction, count)
    every = lax.all_to_all(sums, "dp", 0, 0, tiled=True)
    step_taken, new_master, weights = finish(perm, bounds, every, master, direction)

    pieces = {0: weights}
    offset = half
    while offset:
        pieces |= {k ^ offset: swap(piece, offset) for k, piece in pieces.items()}
        offset //= 2
    new_weights, step_taken, new_master = place(
        perm, [pieces[k] for k in range(count)], (step_taken, new_master)
    )

    def row(value):
        return value.reshape(1, shard_len)

    return (
        new_weights.reshape(-1),
        row(new_master),
        row(new_first),
        row(new_second),
        row(step_taken),
    )


def solution(mesh):
    rows = P(("section", "dp"), None)
    return jax.shard_map(
        per_device,
        mesh=mesh,
        in_specs=(rows, rows, rows, rows, P("section"), P("section")),
        out_specs=(P("section"), rows, rows, rows, rows),
        check_vma=False,
    )
```

```python
import functools
import math

import jax
import jax.numpy as jnp
from jax import lax
from jax.experimental import pallas as pl
from jax.experimental.pallas import tpu as pltpu
from jax.sharding import PartitionSpec as P


beta_first = 0.9
beta_second = 0.999
first_fix = 1.0 - 0.9**10
second_fix = 1.0 - 0.999**10
adam_eps = 1e-06
norm_eps = 1e-06
decay_rate = 0.01
learn_rate = 0.01

LANES = 128
WIRE_SCALE = 1024.0


ANY = pl.BlockSpec(memory_space=pl.ANY)
SMEM = pl.BlockSpec(memory_space=pltpu.SMEM)
VMEM = pl.BlockSpec(memory_space=pltpu.VMEM)


NEAR_BYTES = 1 << 20


def fits(count, shape, dtype):
    return count * math.prod(shape) * jnp.dtype(dtype).itemsize <= NEAR_BYTES


def near(value):
    return pltpu.with_memory_space_constraint(value, pltpu.VMEM)


def output(shape, dtype):
    kind = pltpu.VMEM if fits(1, shape, dtype) else jax.ShapeDtypeStruct
    return kind(shape, dtype)


def fetch_kernel(
    perm_hbm, grads_ref, given_ref, kept_ref, rows_ref, perm_ref, owner_ref, perm_sem, sems
):
    count = rows_ref.shape[0]
    _, shard_rows, _ = given_ref.shape
    shard_len = shard_rows * LANES
    me = lax.axis_index("dp")

    def fetch(block):
        return pltpu.make_async_copy(
            grads_ref.at[:, pl.ds(block * shard_len, shard_len)], rows_ref.at[block], sems.at[block]
        )

    indices = pltpu.make_async_copy(perm_hbm, perm_ref, perm_sem)
    indices.start()
    for block in range(count):
        fetch(block).start()
    indices.wait()
    for device in range(count):
        owner_ref[perm_ref[device]] = device
    for block in range(count):
        offset = owner_ref[block] ^ me
        fetch(block).wait()

        @pl.when(offset & 1 == 1)
        def _():
            given_ref[offset >> 1] = rows_ref[block].reshape(shard_rows, LANES)

        @pl.when(offset & 1 == 0)
        def _():
            kept_ref[offset >> 1] = rows_ref[block].reshape(shard_rows, LANES)


def fetch_blocks(grads, perm, shard_len):
    count = perm.shape[0]
    half = output((count // 2, shard_len // LANES, LANES), grads.dtype)
    return pl.pallas_call(
        fetch_kernel,
        out_shape=(half, half),
        in_specs=[ANY, ANY],
        out_specs=(VMEM, VMEM),
        scratch_shapes=[
            pltpu.VMEM((count, 1, shard_len), grads.dtype),
            pltpu.SMEM(perm.shape, perm.dtype),
            pltpu.SMEM(perm.shape, perm.dtype),
            pltpu.SemaphoreType.DMA,
            pltpu.SemaphoreType.DMA((count,)),
        ],
        name="fetch_blocks",
    )(perm, grads)


def members_kernel(perm_ref, bounds_ref, master_ref, rows_ref, columns_ref, weight_ref):
    tensors = bounds_ref.shape[0] - 1
    shard_rows = master_ref.shape[0]
    me = lax.axis_index("dp")
    half = lax.axis_size("dp") // 2

    def one_hot(shape, tensor_dim, device):
        first = perm_ref[device] * shard_rows
        tensor = lax.broadcasted_iota(jnp.int32, shape, tensor_dim)
        row = lax.broadcasted_iota(jnp.int32, shape, 1 - tensor_dim)
        low = jnp.zeros(shape, jnp.int32)
        high = jnp.zeros(shape, jnp.int32)
        for t in range(tensors):
            low = jnp.where(tensor == t, bounds_ref[t] // LANES - first, low)
            high = jnp.where(tensor == t, bounds_ref[t + 1] // LANES - first, high)
        return ((row >= low) & (row < high)).astype(jnp.float32)

    rows_ref[0] = one_hot((shard_rows, tensors), 1, me)
    rows_ref[1] = one_hot((shard_rows, tensors), 1, me ^ half)
    columns = one_hot((tensors, shard_rows), 0, me)
    columns_ref[...] = columns
    weight_ref[...] = square_sums(columns, master_ref[...])


def exact_dot(left, right):
    return jnp.dot(
        left, right, precision=lax.Precision.HIGHEST, preferred_element_type=jnp.float32
    )


def square_sums(columns, value):
    return jnp.sum(exact_dot(columns, value * value), axis=1, keepdims=True)


def find_members(perm, bounds, master):
    tensors = bounds.shape[0] - 1
    shard_rows = master.shape[0]
    return pl.pallas_call(
        members_kernel,
        out_shape=(
            output((2, shard_rows, tensors), jnp.float32),
            output((tensors, shard_rows), jnp.float32),
            output((tensors, 1), jnp.float32),
        ),
        in_specs=[SMEM, SMEM, VMEM],
        out_specs=(VMEM, VMEM, VMEM),
        name="find_members",
    )(perm, bounds, near(master))


def sums_kernel(columns_ref, weight_ref, direction_ref, out_ref):
    update_sq = square_sums(columns_ref[...], direction_ref[...])
    lane = lax.broadcasted_iota(jnp.int32, out_ref.shape, 1)
    out_ref[...] = jnp.where(lane == 0, weight_ref[...], jnp.where(lane == 1, update_sq, 0.0))


def tensor_sums(columns, weight_sq, direction):
    return pl.pallas_call(
        sums_kernel,
        out_shape=output((columns.shape[0], LANES), jnp.float32),
        in_specs=[VMEM, VMEM, VMEM],
        out_specs=VMEM,
        name="tensor_sums",
    )(near(columns), near(weight_sq), near(direction))


def finish_kernel(
    rows_ref, sums_ref, masters_refs, directions_refs, step_ref, new_ref, weights_ref
):
    norms = jnp.sqrt(sums_ref[...])
    ratios = norms[:, 0:1] / (norms[:, 1:2] + norm_eps)
    ratios = jnp.broadcast_to(ratios, norms.shape)
    for k in range(2):
        step = exact_dot(rows_ref[k], ratios) * directions_refs[k][...]
        new = masters_refs[k][...] - learn_rate * step
        weights_ref[k] = new.astype(jnp.bfloat16)
        if k == 0:
            step_ref[...] = step
            new_ref[...] = new


def finish(rows, sums, masters, directions):
    like = output(masters[0].shape, jnp.float32)
    weights = output((2, *masters[0].shape), jnp.bfloat16)
    return pl.pallas_call(
        finish_kernel,
        out_shape=(like, like, weights),
        in_specs=[VMEM, VMEM, (VMEM, VMEM), (VMEM, VMEM)],
        out_specs=(VMEM, VMEM, VMEM),
        name="finish",
    )(near(rows), near(sums), tuple(map(near, masters)), tuple(map(near, directions)))


def block_of(perm, device):
    lane = lax.broadcasted_iota(jnp.int32, perm.shape, 1)
    return jnp.sum(jnp.where(lane == device, perm, 0.0)).astype(jnp.int32)


def place_kernel(offsets, extra, perm_ref, *refs):
    count = len(offsets)
    sems = refs[-1]
    pieces, kept = refs[:count], refs[count : count + extra]
    out_ref, rows_out = refs[-2 - extra], refs[-1 - extra : -1]
    me = lax.axis_index("dp")
    copies = [
        pltpu.make_async_copy(source, target, sems.at[k])
        for k, (source, target) in enumerate(zip(kept, rows_out))
    ]
    for copy in copies:
        copy.start()
    perm = perm_ref[...]
    half = perm.shape[1] // 2
    for k, offset in enumerate((*offsets, *(offset ^ half for offset in offsets))):
        source = pieces[k % count].at[k // count]
        block = block_of(perm, me ^ offset)
        copies.append(pltpu.make_async_copy(source, out_ref.at[block], sems.at[extra + k]))
        copies[-1].start()
    for copy in copies:
        copy.wait()


def place(perm, pieces, rows, into=None):
    offsets = tuple(pieces)
    pieces = tuple(pieces.values())
    count = len(pieces)
    like = pieces[0]
    close = fits(count, like.shape, like.dtype)
    operands = (perm, *(map(near, pieces) if close else pieces), *map(near, rows))
    in_specs = [VMEM] + [VMEM if close else ANY] * count + [VMEM] * len(rows)
    aliases = {}
    if into is not None:
        aliases = {len(operands): 0}
        operands += (into,)
        in_specs.append(ANY)
    return pl.pallas_call(
        functools.partial(place_kernel, offsets, len(rows)),
        out_shape=(
            jax.ShapeDtypeStruct((perm.shape[1], *like.shape[1:]), like.dtype),
            *(jax.ShapeDtypeStruct(row.shape, row.dtype) for row in rows),
        ),
        in_specs=in_specs,
        out_specs=(ANY,) * (1 + len(rows)),
        scratch_shapes=[pltpu.SemaphoreType.DMA((2 * count + len(rows),))],
        input_output_aliases=aliases,
        name="place",
    )(*operands)


def offset_groups(high):
    groups = []
    while high > 2:
        low = max(high // 4, 2)
        groups.append(sorted((k * low for k in range(1, high // low)), key=lambda hop: hop == low))
        high = low
    return groups


def sum_groups(high):
    groups = []
    low = 2
    while low < high:
        end = min(low * 4, high)
        groups.append([k * low for k in range(1, end // low)])
        low = end
    return groups


def gather_plan(count):
    known = [0]
    stages = []
    for group in offset_groups(count // 2) + [[1]]:
        stages.append([(piece, hop) for hop in group for piece in known])
        known += sorted(piece ^ hop for piece, hop in stages[-1])
    order = []
    for piece in known:
        for stage in stages:
            order += [exchange for exchange in stage if exchange[0] == piece]
    return order


def reduce_plan(half):
    far = range(half // 2, half)
    by_way = [k for k in far if k % 2]
    onward = [k for k in far if k % 2 == 0]
    close = list(range(half // 2 - 1, 0, -1))
    return by_way, close[:1] + onward + close[1:]


def per_device(grads, master, first_moment, second_moment, perm, bounds):
    count = lax.axis_size("dp")
    if count & (count - 1):
        raise ValueError("unsupported dp size")
    half = count // 2
    shard_len = master.shape[1]
    shard_rows = shard_len // LANES

    def swap(value, offset):
        return lax.ppermute(value, "dp", [(i, i ^ offset) for i in range(count)])

    master = master.reshape(shard_rows, LANES)
    first_moment = first_moment.reshape(shard_rows, LANES)
    second_moment = second_moment.reshape(shard_rows, LANES)

    perm_row = near(perm.astype(jnp.float32)[None])

    given, kept = fetch_blocks(grads, perm, shard_len)
    taken = swap(given, 1)
    far_master = swap(master, half)
    rows, columns, weight_sq = find_members(perm, bounds, master)

    def send(value, offset):
        return swap((value * WIRE_SCALE).astype(jnp.float16), offset)

    pairs = [kept[k].astype(jnp.float32) + taken[k].astype(jnp.float32) for k in range(half)]
    total = pairs[0]
    by_way, straight = reduce_plan(half)
    for k in by_way:
        added = send(pairs[k], 2)
        pairs[k ^ 1] = pairs[k ^ 1] + added.astype(jnp.float32) * (1.0 / WIRE_SCALE)
    arrived = [send(pairs[k], 2 * k) for k in straight]
    for piece in arrived:
        total = total + piece.astype(jnp.float32) * (1.0 / WIRE_SCALE)
    own_grad = total / count

    new_first = beta_first * first_moment + (1.0 - beta_first) * own_grad
    new_second = beta_second * second_moment + (1.0 - beta_second) * own_grad * own_grad
    direction = (
        new_first / first_fix / (jnp.sqrt(new_second / second_fix) + adam_eps) + decay_rate * master
    )
    far_direction = swap(direction, half)
    sums = tensor_sums(columns, weight_sq, direction)
    sums = sums + swap(sums, 1)
    for group in sum_groups(half):
        parts = [sums] + [swap(sums, hop) for hop in group]
        while len(parts) > 1:
            parts = [low + high for low, high in zip(parts[::2], parts[1::2])]
        (sums,) = parts
    sums = sums + swap(sums, half)
    step_taken, new_master, weights = finish(
        rows, sums, (master, far_master), (direction, far_direction)
    )

    pieces = {0: weights}
    for piece, hop in gather_plan(count):
        pieces[piece ^ hop] = swap(pieces[piece], hop)
    new_weights, step_taken, new_master = place(
        perm_row, {k: pieces[k] for k in range(0, half, 2)}, (step_taken, new_master)
    )
    (new_weights,) = place(perm_row, {k: pieces[k] for k in range(1, half, 2)}, (), new_weights)

    def row(value):
        return value.reshape(1, shard_len)

    return (
        new_weights.reshape(-1),
        row(new_master),
        row(new_first),
        row(new_second),
        row(step_taken),
    )


def solution(mesh):
    rows = P(("section", "dp"), None)

    return jax.shard_map(
        per_device,
        mesh=mesh,
        in_specs=(rows, rows, rows, rows, P("section"), P("section")),
        out_specs=(P("section"), rows, rows, rows, rows),
        check_vma=False,
    )
```

```python
import functools
import math

import jax
import jax.numpy as jnp
from jax import lax
from jax.experimental import pallas as pl
from jax.experimental.pallas import tpu as pltpu
from jax.sharding import PartitionSpec as P


beta_first = 0.9
beta_second = 0.999
first_fix = 1.0 - 0.9**10
second_fix = 1.0 - 0.999**10
adam_eps = 1e-06
norm_eps = 1e-06
decay_rate = 0.01
learn_rate = 0.01

LANES = 128
WIRE_SCALE = 1024.0


ANY = pl.BlockSpec(memory_space=pl.ANY)
SMEM = pl.BlockSpec(memory_space=pltpu.SMEM)
VMEM = pl.BlockSpec(memory_space=pltpu.VMEM)


NEAR_BYTES = 1 << 20


def fits(count, shape, dtype):
    return count * math.prod(shape) * jnp.dtype(dtype).itemsize <= NEAR_BYTES


def near(value):
    return pltpu.with_memory_space_constraint(value, pltpu.VMEM)


def output(shape, dtype):
    kind = pltpu.VMEM if fits(1, shape, dtype) else jax.ShapeDtypeStruct
    return kind(shape, dtype)


def fetch_kernel(
    perm_hbm,
    grads_ref,
    given_far_ref,
    given_ref,
    kept_far_ref,
    kept_ref,
    rows_ref,
    perm_ref,
    owner_ref,
    perm_sem,
    sems,
):
    count = rows_ref.shape[0]
    quarter = count // 4
    _, shard_rows, _ = given_ref.shape
    shard_len = shard_rows * LANES
    me = lax.axis_index("dp")

    def fetch(block):
        return pltpu.make_async_copy(
            grads_ref.at[:, pl.ds(block * shard_len, shard_len)], rows_ref.at[block], sems.at[block]
        )

    indices = pltpu.make_async_copy(perm_hbm, perm_ref, perm_sem)
    indices.start()
    for block in range(count):
        fetch(block).start()
    indices.wait()
    for device in range(count):
        owner_ref[perm_ref[device]] = device
    for block in range(count):
        offset = owner_ref[block] ^ me
        chip = offset >> 1
        by_way = (chip >= quarter) & (chip & 1 == 1)
        past = (chip - quarter) >> 1
        slot = jnp.where(by_way, past, jnp.where(chip < quarter, chip, quarter + past))
        fetch(block).wait()
        for flip, way, out_ref in (
            (1, True, given_far_ref),
            (1, False, given_ref),
            (0, True, kept_far_ref),
            (0, False, kept_ref),
        ):

            @pl.when((offset & 1 == flip) & (by_way == way))
            def _():
                out_ref[slot] = rows_ref[block].reshape(shard_rows, LANES)


def fetch_blocks(grads, perm, shard_len):
    count = perm.shape[0]
    far, rest = (
        output((size, shard_len // LANES, LANES), grads.dtype)
        for size in (count // 8, count // 2 - count // 8)
    )
    outs = pl.pallas_call(
        fetch_kernel,
        out_shape=(far, rest, far, rest),
        in_specs=[ANY, ANY],
        out_specs=(VMEM,) * 4,
        scratch_shapes=[
            pltpu.VMEM((count, 1, shard_len), grads.dtype),
            pltpu.SMEM(perm.shape, perm.dtype),
            pltpu.SMEM(perm.shape, perm.dtype),
            pltpu.SemaphoreType.DMA,
            pltpu.SemaphoreType.DMA((count,)),
        ],
        name="fetch_blocks",
    )(perm, grads)
    return outs[:2], outs[2:]


def members_kernel(perm_ref, bounds_ref, master_ref, rows_ref, columns_ref, weight_ref):
    tensors = bounds_ref.shape[0] - 1
    shard_rows = master_ref.shape[0]
    me = lax.axis_index("dp")
    half = lax.axis_size("dp") // 2

    def one_hot(shape, tensor_dim, device):
        first = perm_ref[device] * shard_rows
        tensor = lax.broadcasted_iota(jnp.int32, shape, tensor_dim)
        row = lax.broadcasted_iota(jnp.int32, shape, 1 - tensor_dim)
        low = jnp.zeros(shape, jnp.int32)
        high = jnp.zeros(shape, jnp.int32)
        for t in range(tensors):
            low = jnp.where(tensor == t, bounds_ref[t] // LANES - first, low)
            high = jnp.where(tensor == t, bounds_ref[t + 1] // LANES - first, high)
        return ((row >= low) & (row < high)).astype(jnp.float32)

    rows_ref[0] = one_hot((shard_rows, tensors), 1, me)
    rows_ref[1] = one_hot((shard_rows, tensors), 1, me ^ half)
    columns = one_hot((tensors, shard_rows), 0, me)
    columns_ref[...] = columns
    weight_ref[...] = square_sums(columns, master_ref[...])


def exact_dot(left, right):
    return jnp.dot(
        left, right, precision=lax.Precision.HIGHEST, preferred_element_type=jnp.float32
    )


def square_sums(columns, value):
    return jnp.sum(exact_dot(columns, value * value), axis=1, keepdims=True)


def find_members(perm, bounds, master):
    tensors = bounds.shape[0] - 1
    shard_rows = master.shape[0]
    return pl.pallas_call(
        members_kernel,
        out_shape=(
            output((2, shard_rows, tensors), jnp.float32),
            output((tensors, shard_rows), jnp.float32),
            output((tensors, 1), jnp.float32),
        ),
        in_specs=[SMEM, SMEM, VMEM],
        out_specs=(VMEM, VMEM, VMEM),
        name="find_members",
    )(perm, bounds, near(master))


def sums_kernel(columns_ref, weight_ref, direction_ref, out_ref):
    update_sq = square_sums(columns_ref[...], direction_ref[...])
    lane = lax.broadcasted_iota(jnp.int32, out_ref.shape, 1)
    out_ref[...] = jnp.where(lane == 0, weight_ref[...], jnp.where(lane == 1, update_sq, 0.0))


def tensor_sums(columns, weight_sq, direction):
    return pl.pallas_call(
        sums_kernel,
        out_shape=output((columns.shape[0], LANES), jnp.float32),
        in_specs=[VMEM, VMEM, VMEM],
        out_specs=VMEM,
        name="tensor_sums",
    )(near(columns), near(weight_sq), near(direction))


def finish_kernel(
    rows_ref, sums_ref, masters_refs, directions_refs, step_ref, new_ref, weights_ref
):
    norms = jnp.sqrt(sums_ref[...])
    ratios = norms[:, 0:1] / (norms[:, 1:2] + norm_eps)
    ratios = jnp.broadcast_to(ratios, norms.shape)
    for k in range(2):
        step = exact_dot(rows_ref[k], ratios) * directions_refs[k][...]
        new = masters_refs[k][...] - learn_rate * step
        weights_ref[k] = new.astype(jnp.bfloat16)
        if k == 0:
            step_ref[...] = step
            new_ref[...] = new


def finish(rows, sums, masters, directions):
    like = output(masters[0].shape, jnp.float32)
    weights = output((2, *masters[0].shape), jnp.bfloat16)
    return pl.pallas_call(
        finish_kernel,
        out_shape=(like, like, weights),
        in_specs=[VMEM, VMEM, (VMEM, VMEM), (VMEM, VMEM)],
        out_specs=(VMEM, VMEM, VMEM),
        name="finish",
    )(near(rows), near(sums), tuple(map(near, masters)), tuple(map(near, directions)))


def block_of(perm, device):
    lane = lax.broadcasted_iota(jnp.int32, perm.shape, 1)
    return jnp.sum(jnp.where(lane == device, perm, 0.0)).astype(jnp.int32)


def place_kernel(offsets, extra, perm_ref, *refs):
    count = len(offsets)
    sems = refs[-1]
    pieces, kept = refs[:count], refs[count : count + extra]
    out_ref, rows_out = refs[-2 - extra], refs[-1 - extra : -1]
    me = lax.axis_index("dp")
    copies = [
        pltpu.make_async_copy(source, target, sems.at[k])
        for k, (source, target) in enumerate(zip(kept, rows_out))
    ]
    for copy in copies:
        copy.start()
    perm = perm_ref[...]
    half = perm.shape[1] // 2
    for k, offset in enumerate((*offsets, *(offset ^ half for offset in offsets))):
        source = pieces[k % count].at[k // count]
        block = block_of(perm, me ^ offset)
        copies.append(pltpu.make_async_copy(source, out_ref.at[block], sems.at[extra + k]))
        copies[-1].start()
    for copy in copies:
        copy.wait()


def place(perm, pieces, rows, into=None):
    offsets = tuple(pieces)
    pieces = tuple(pieces.values())
    count = len(pieces)
    like = pieces[0]
    close = fits(count, like.shape, like.dtype)
    operands = (perm, *(map(near, pieces) if close else pieces), *map(near, rows))
    in_specs = [VMEM] + [VMEM if close else ANY] * count + [VMEM] * len(rows)
    aliases = {}
    if into is not None:
        aliases = {len(operands): 0}
        operands += (into,)
        in_specs.append(ANY)
    return pl.pallas_call(
        functools.partial(place_kernel, offsets, len(rows)),
        out_shape=(
            jax.ShapeDtypeStruct((perm.shape[1], *like.shape[1:]), like.dtype),
            *(jax.ShapeDtypeStruct(row.shape, row.dtype) for row in rows),
        ),
        in_specs=in_specs,
        out_specs=(ANY,) * (1 + len(rows)),
        scratch_shapes=[pltpu.SemaphoreType.DMA((2 * count + len(rows),))],
        input_output_aliases=aliases,
        name="place",
    )(*operands)


def offset_groups(high):
    groups = []
    while high > 2:
        low = max(high // 4, 2)
        hops = [k * low for k in range(1, high // low)]
        groups.append(hops[1:2] + hops[:1] + hops[2:])
        high = low
    return groups


def sum_groups(high):
    groups = []
    low = 2
    while low < high:
        end = min(low * 4, high)
        groups.append([k * low for k in range(end // low - 1, 0, -1)])
        low = end
    return groups


def gather_plan(count):
    known = [0]
    stages = []
    for group in offset_groups(count // 2) + [[1]]:
        stages.append([(piece, hop) for hop in group for piece in known])
        known += sorted(piece ^ hop for piece, hop in stages[-1])
    order = []
    for piece in known:
        for stage in stages:
            order += [exchange for exchange in stage if exchange[0] == piece]
    return order


def reduce_plan(half):
    far = range(half // 2, half)
    by_way = [k for k in far if k % 2]
    onward = [k for k in far if k % 2 == 0]
    close = list(range(half // 2 - 1, 0, -1))
    return by_way, close[:-1] + onward + close[-1:]


def per_device(grads, master, first_moment, second_moment, perm, bounds):
    count = lax.axis_size("dp")
    if count & (count - 1):
        raise ValueError("unsupported dp size")
    half = count // 2
    shard_len = master.shape[1]
    shard_rows = shard_len // LANES

    def swap(value, offset):
        return lax.ppermute(value, "dp", [(i, i ^ offset) for i in range(count)])

    master = master.reshape(shard_rows, LANES)
    first_moment = first_moment.reshape(shard_rows, LANES)
    second_moment = second_moment.reshape(shard_rows, LANES)

    perm_row = near(perm.astype(jnp.float32)[None])

    given, kept = fetch_blocks(grads, perm, shard_len)
    by_way, straight = reduce_plan(half)
    groups = (by_way, [k for k in range(half) if k not in by_way])
    taken = [swap(value, 1) for value in given]
    far_master = swap(master, half)
    rows, columns, weight_sq = find_members(perm, bounds, master)

    def wire(value):
        return (value * WIRE_SCALE).astype(jnp.float16)

    def unwire(value):
        return value.astype(jnp.float32) * (1.0 / WIRE_SCALE)

    def pair_sums(index):
        return {
            k: kept[index][slot].astype(jnp.float32) + taken[index][slot].astype(jnp.float32)
            for slot, k in enumerate(groups[index])
        }

    leaving = [wire(value) for value in pair_sums(0).values()]
    added = {k ^ 1: swap(value, 2) for k, value in zip(by_way, leaving)}
    taken[1], _ = lax.optimization_barrier((taken[1], leaving[-1]))
    pairs = pair_sums(1)
    for k, value in added.items():
        pairs[k] = pairs[k] + unwire(value)
    total = pairs[0]
    arrived = [swap(wire(pairs[k]), 2 * k) for k in straight]
    for piece in arrived:
        total = total + unwire(piece)
    own_grad = total / count

    new_first = beta_first * first_moment + (1.0 - beta_first) * own_grad
    new_second = beta_second * second_moment + (1.0 - beta_second) * own_grad * own_grad
    direction = (
        new_first / first_fix / (jnp.sqrt(new_second / second_fix) + adam_eps) + decay_rate * master
    )
    sums = tensor_sums(columns, weight_sq, direction)
    sums = sums + swap(sums, half)
    far_direction = swap(direction, half)
    sums = sums + swap(sums, 1)
    for group in sum_groups(half):
        parts = [sums] + [swap(sums, hop) for hop in group][::-1]
        while len(parts) > 1:
            parts = [low + high for low, high in zip(parts[::2], parts[1::2])]
        (sums,) = parts
    step_taken, new_master, weights = finish(
        rows, sums, (master, far_master), (direction, far_direction)
    )

    pieces = {0: weights}
    for piece, hop in gather_plan(count):
        pieces[piece ^ hop] = swap(pieces[piece], hop)
    last = [k for k in sorted(pieces) if k % 2][len(pieces) // 4 :]
    new_weights, step_taken, new_master, new_first, new_second = place(
        perm_row,
        {k: piece for k, piece in pieces.items() if k not in last},
        (step_taken, new_master, new_first, new_second),
    )
    (new_weights,) = place(perm_row, {k: pieces[k] for k in last}, (), new_weights)

    def row(value):
        return value.reshape(1, shard_len)

    return (
        new_weights.reshape(-1),
        row(new_master),
        row(new_first),
        row(new_second),
        row(step_taken),
    )


def solution(mesh):
    rows = P(("section", "dp"), None)

    return jax.shard_map(
        per_device,
        mesh=mesh,
        in_specs=(rows, rows, rows, rows, P("section"), P("section")),
        out_specs=(P("section"), rows, rows, rows, rows),
        check_vma=False,
    )
```

```python
import functools
import math

import jax
import jax.numpy as jnp
from jax import lax
from jax.experimental import pallas as pl
from jax.experimental.pallas import tpu as pltpu
from jax.sharding import PartitionSpec as P


beta_first = 0.9
beta_second = 0.999
first_fix = 1.0 - 0.9**10
second_fix = 1.0 - 0.999**10
adam_eps = 1e-06
norm_eps = 1e-06
decay_rate = 0.01
learn_rate = 0.01

LANES = 128
WIRE_SCALE = 1024.0


ANY = pl.BlockSpec(memory_space=pl.ANY)
SMEM = pl.BlockSpec(memory_space=pltpu.SMEM)
VMEM = pl.BlockSpec(memory_space=pltpu.VMEM)


NEAR_BYTES = 1 << 20


def fits(count, shape, dtype):
    return count * math.prod(shape) * jnp.dtype(dtype).itemsize <= NEAR_BYTES


def near(value):
    return pltpu.with_memory_space_constraint(value, pltpu.VMEM)


def output(shape, dtype):
    kind = pltpu.VMEM if fits(1, shape, dtype) else jax.ShapeDtypeStruct
    return kind(shape, dtype)


def fetch_kernel(
    perm_hbm,
    grads_ref,
    given_far_ref,
    given_ref,
    kept_far_ref,
    kept_ref,
    rows_ref,
    perm_ref,
    owner_ref,
    perm_sem,
    sems,
):
    count = rows_ref.shape[0]
    quarter = count // 4
    _, shard_rows, _ = given_ref.shape
    shard_len = shard_rows * LANES
    me = lax.axis_index("dp")

    def fetch(block):
        return pltpu.make_async_copy(
            grads_ref.at[:, pl.ds(block * shard_len, shard_len)], rows_ref.at[block], sems.at[block]
        )

    indices = pltpu.make_async_copy(perm_hbm, perm_ref, perm_sem)
    indices.start()
    for block in range(count):
        fetch(block).start()
    indices.wait()
    for device in range(count):
        owner_ref[perm_ref[device]] = device
    for block in range(count):
        offset = owner_ref[block] ^ me
        chip = offset >> 1
        by_way = (chip >= quarter) & (chip & 1 == 1)
        past = (chip - quarter) >> 1
        slot = jnp.where(by_way, past, jnp.where(chip < quarter, chip, quarter + past))
        fetch(block).wait()

        def put(far_ref, rest_ref):
            def into(out_ref):
                out_ref[slot] = rows_ref[block].reshape(shard_rows, LANES)

            lax.cond(by_way, lambda: into(far_ref), lambda: into(rest_ref))

        lax.cond(
            offset & 1 == 1,
            lambda: put(given_far_ref, given_ref),
            lambda: put(kept_far_ref, kept_ref),
        )


def fetch_blocks(grads, perm, shard_len):
    count = perm.shape[0]
    far, rest = (
        output((size, shard_len // LANES, LANES), grads.dtype)
        for size in (count // 8, count // 2 - count // 8)
    )
    outs = pl.pallas_call(
        fetch_kernel,
        out_shape=(far, rest, far, rest),
        in_specs=[ANY, ANY],
        out_specs=(VMEM,) * 4,
        scratch_shapes=[
            pltpu.VMEM((count, 1, shard_len), grads.dtype),
            pltpu.SMEM(perm.shape, perm.dtype),
            pltpu.SMEM(perm.shape, perm.dtype),
            pltpu.SemaphoreType.DMA,
            pltpu.SemaphoreType.DMA((count,)),
        ],
        name="fetch_blocks",
    )(perm, grads)
    return outs[:2], outs[2:]


def members_kernel(perm_ref, bounds_ref, master_ref, rows_ref, columns_ref, weight_ref):
    tensors = bounds_ref.shape[0] - 1
    shard_rows = master_ref.shape[0]
    me = lax.axis_index("dp")
    half = lax.axis_size("dp") // 2

    def one_hot(shape, tensor_dim, device):
        first = perm_ref[device] * shard_rows
        tensor = lax.broadcasted_iota(jnp.int32, shape, tensor_dim)
        row = lax.broadcasted_iota(jnp.int32, shape, 1 - tensor_dim)
        low = jnp.zeros(shape, jnp.int32)
        high = jnp.zeros(shape, jnp.int32)
        for t in range(tensors):
            low = jnp.where(tensor == t, bounds_ref[t] // LANES - first, low)
            high = jnp.where(tensor == t, bounds_ref[t + 1] // LANES - first, high)
        return ((row >= low) & (row < high)).astype(jnp.float32)

    rows_ref[0] = one_hot((shard_rows, tensors), 1, me)
    rows_ref[1] = one_hot((shard_rows, tensors), 1, me ^ half)
    columns = one_hot((tensors, shard_rows), 0, me)
    columns_ref[...] = columns
    weight_ref[...] = square_sums(columns, master_ref[...])


def exact_dot(left, right):
    return jnp.dot(
        left, right, precision=lax.Precision.HIGHEST, preferred_element_type=jnp.float32
    )


def square_sums(columns, value):
    return jnp.sum(exact_dot(columns, value * value), axis=1, keepdims=True)


def find_members(perm, bounds, master):
    tensors = bounds.shape[0] - 1
    shard_rows = master.shape[0]
    return pl.pallas_call(
        members_kernel,
        out_shape=(
            output((2, shard_rows, tensors), jnp.float32),
            output((tensors, shard_rows), jnp.float32),
            output((tensors, 1), jnp.float32),
        ),
        in_specs=[SMEM, SMEM, VMEM],
        out_specs=(VMEM, VMEM, VMEM),
        name="find_members",
    )(perm, bounds, near(master))


def sums_kernel(columns_ref, weight_ref, direction_ref, out_ref):
    update_sq = square_sums(columns_ref[...], direction_ref[...])
    lane = lax.broadcasted_iota(jnp.int32, out_ref.shape, 1)
    out_ref[...] = jnp.where(lane == 0, weight_ref[...], jnp.where(lane == 1, update_sq, 0.0))


def tensor_sums(columns, weight_sq, direction):
    return pl.pallas_call(
        sums_kernel,
        out_shape=output((columns.shape[0], LANES), jnp.float32),
        in_specs=[VMEM, VMEM, VMEM],
        out_specs=VMEM,
        name="tensor_sums",
    )(near(columns), near(weight_sq), near(direction))


def finish_kernel(
    rows_ref, sums_ref, masters_refs, directions_refs, step_ref, new_ref, weights_ref
):
    norms = jnp.sqrt(sums_ref[...])
    ratios = norms[:, 0:1] / (norms[:, 1:2] + norm_eps)
    ratios = jnp.broadcast_to(ratios, norms.shape)
    for k in range(2):
        step = exact_dot(rows_ref[k], ratios) * directions_refs[k][...]
        new = masters_refs[k][...] - learn_rate * step
        weights_ref[k] = new.astype(jnp.bfloat16)
        if k == 0:
            step_ref[...] = step
            new_ref[...] = new


def finish(rows, sums, masters, directions):
    like = output(masters[0].shape, jnp.float32)
    weights = output((2, *masters[0].shape), jnp.bfloat16)
    return pl.pallas_call(
        finish_kernel,
        out_shape=(like, like, weights),
        in_specs=[VMEM, VMEM, (VMEM, VMEM), (VMEM, VMEM)],
        out_specs=(VMEM, VMEM, VMEM),
        name="finish",
    )(near(rows), near(sums), tuple(map(near, masters)), tuple(map(near, directions)))


def block_of(perm, device):
    lane = lax.broadcasted_iota(jnp.int32, perm.shape, 1)
    return jnp.sum(jnp.where(lane == device, perm, 0.0)).astype(jnp.int32)


def place_kernel(offsets, extra, perm_ref, *refs):
    count = len(offsets)
    sems = refs[-1]
    pieces, kept = refs[:count], refs[count : count + extra]
    out_ref, rows_out = refs[-2 - extra], refs[-1 - extra : -1]
    me = lax.axis_index("dp")
    copies = [
        pltpu.make_async_copy(source, target, sems.at[k])
        for k, (source, target) in enumerate(zip(kept, rows_out))
    ]
    for copy in copies:
        copy.start()
    perm = perm_ref[...]
    half = perm.shape[1] // 2
    for k, offset in enumerate((*offsets, *(offset ^ half for offset in offsets))):
        source = pieces[k % count].at[k // count]
        block = block_of(perm, me ^ offset)
        copies.append(pltpu.make_async_copy(source, out_ref.at[block], sems.at[extra + k]))
        copies[-1].start()
    for copy in copies:
        copy.wait()


def place(perm, pieces, rows, into=None):
    offsets = tuple(pieces)
    pieces = tuple(pieces.values())
    count = len(pieces)
    like = pieces[0]
    close = fits(count, like.shape, like.dtype)
    operands = (perm, *(map(near, pieces) if close else pieces), *map(near, rows))
    in_specs = [VMEM] + [VMEM if close else ANY] * count + [VMEM] * len(rows)
    aliases = {}
    if into is not None:
        aliases = {len(operands): 0}
        operands += (into,)
        in_specs.append(ANY)
    return pl.pallas_call(
        functools.partial(place_kernel, offsets, len(rows)),
        out_shape=(
            jax.ShapeDtypeStruct((perm.shape[1], *like.shape[1:]), like.dtype),
            *(jax.ShapeDtypeStruct(row.shape, row.dtype) for row in rows),
        ),
        in_specs=in_specs,
        out_specs=(ANY,) * (1 + len(rows)),
        scratch_shapes=[pltpu.SemaphoreType.DMA((2 * count + len(rows),))],
        input_output_aliases=aliases,
        name="place",
    )(*operands)


def offset_groups(high):
    groups = []
    while high > 2:
        low = max(high // 4, 2)
        hops = [k * low for k in range(1, high // low)]
        groups.append(hops[1:2] + hops[:1] + hops[2:])
        high = low
    return groups


def sum_groups(high):
    groups = []
    low = 2
    while low < high:
        end = min(low * 4, high)
        groups.append([k * low for k in range(end // low - 1, 0, -1)])
        low = end
    return groups


def gather_plan(count):
    known = [0]
    stages = []
    for group in offset_groups(count // 2) + [[1]]:
        stages.append([(piece, hop) for hop in group for piece in known])
        known += sorted(piece ^ hop for piece, hop in stages[-1])
    order = []
    for piece in known:
        for stage in stages:
            order += [exchange for exchange in stage if exchange[0] == piece]
    return order


def reduce_plan(half):
    far = range(half // 2, half)
    by_way = [k for k in far if k % 2]
    onward = [k for k in far if k % 2 == 0]
    close = list(range(half // 2 - 1, 0, -1))
    return by_way, close[:-1] + onward[::-1] + close[-1:]


def per_device(grads, master, first_moment, second_moment, perm, bounds):
    count = lax.axis_size("dp")
    if count & (count - 1):
        raise ValueError("unsupported dp size")
    half = count // 2
    shard_len = master.shape[1]
    shard_rows = shard_len // LANES

    def swap(value, offset):
        return lax.ppermute(value, "dp", [(i, i ^ offset) for i in range(count)])

    master = master.reshape(shard_rows, LANES)
    first_moment = first_moment.reshape(shard_rows, LANES)
    second_moment = second_moment.reshape(shard_rows, LANES)

    perm_row = near(perm.astype(jnp.float32)[None])

    given, kept = fetch_blocks(grads, perm, shard_len)
    by_way, straight = reduce_plan(half)
    groups = (by_way, [k for k in range(half) if k not in by_way])
    taken = [swap(value, 1) for value in given]
    far_master = swap(master, half)
    rows, columns, weight_sq = find_members(perm, bounds, master)

    def wire(value):
        return (value * WIRE_SCALE).astype(jnp.float16)

    def unwire(value):
        return value.astype(jnp.float32) * (1.0 / WIRE_SCALE)

    def pair_sums(index):
        return {
            k: kept[index][slot].astype(jnp.float32) + taken[index][slot].astype(jnp.float32)
            for slot, k in enumerate(groups[index])
        }

    leaving = [wire(value) for value in pair_sums(0).values()]
    added = {k ^ 1: swap(value, 2) for k, value in zip(by_way, leaving)}
    taken[1], _ = lax.optimization_barrier((taken[1], leaving[-1]))
    pairs = pair_sums(1)
    for k, value in added.items():
        pairs[k] = pairs[k] + unwire(value)
    total = pairs[0]
    arrived = [swap(wire(pairs[k]), 2 * k) for k in straight]
    for piece in arrived:
        total = total + unwire(piece)
    own_grad = total / count

    new_first = beta_first * first_moment + (1.0 - beta_first) * own_grad
    new_second = beta_second * second_moment + (1.0 - beta_second) * own_grad * own_grad
    direction = (
        new_first / first_fix / (jnp.sqrt(new_second / second_fix) + adam_eps) + decay_rate * master
    )
    sums = tensor_sums(columns, weight_sq, direction)
    sums = sums + swap(sums, half)
    far_direction = swap(direction, half)
    sums = sums + swap(sums, 1)
    for group in sum_groups(half):
        parts = [sums] + [swap(sums, hop) for hop in group][::-1]
        while len(parts) > 1:
            parts = [low + high for low, high in zip(parts[::2], parts[1::2])]
        (sums,) = parts
    step_taken, new_master, weights = finish(
        rows, sums, (master, far_master), (direction, far_direction)
    )

    pieces = {0: weights}
    for piece, hop in gather_plan(count):
        pieces[piece ^ hop] = swap(pieces[piece], hop)
    last = [k for k in sorted(pieces) if k % 2][len(pieces) // 4 :]
    new_weights, step_taken, new_master, new_first, new_second = place(
        perm_row,
        {k: piece for k, piece in pieces.items() if k not in last},
        (step_taken, new_master, new_first, new_second),
    )
    (new_weights,) = place(perm_row, {k: pieces[k] for k in last}, (), new_weights)

    def row(value):
        return value.reshape(1, shard_len)

    return (
        new_weights.reshape(-1),
        row(new_master),
        row(new_first),
        row(new_second),
        row(step_taken),
    )


def solution(mesh):
    rows = P(("section", "dp"), None)

    return jax.shard_map(
        per_device,
        mesh=mesh,
        in_specs=(rows, rows, rows, rows, P("section"), P("section")),
        out_specs=(P("section"), rows, rows, rows, rows),
        check_vma=False,
    )
```

```python
import functools
import math

import jax
import jax.numpy as jnp
from jax import lax
from jax.experimental import pallas as pl
from jax.experimental.pallas import tpu as pltpu
from jax.sharding import PartitionSpec as P


beta_first = 0.9
beta_second = 0.999
first_fix = 1.0 - 0.9**10
second_fix = 1.0 - 0.999**10
adam_eps = 1e-06
norm_eps = 1e-06
decay_rate = 0.01
learn_rate = 0.01

LANES = 128
WIRE_SCALE = 1024.0


ANY = pl.BlockSpec(memory_space=pl.ANY)
SMEM = pl.BlockSpec(memory_space=pltpu.SMEM)
VMEM = pl.BlockSpec(memory_space=pltpu.VMEM)


NEAR_BYTES = 1 << 20


def fits(count, shape, dtype):
    return count * math.prod(shape) * jnp.dtype(dtype).itemsize <= NEAR_BYTES


def near(value):
    return pltpu.with_memory_space_constraint(value, pltpu.VMEM)


def output(shape, dtype):
    kind = pltpu.VMEM if fits(1, shape, dtype) else jax.ShapeDtypeStruct
    return kind(shape, dtype)


def fetch_kernel(
    perm_hbm,
    grads_ref,
    given_far_ref,
    given_ref,
    kept_far_ref,
    kept_ref,
    rows_ref,
    perm_ref,
    owner_ref,
    perm_sem,
    sems,
):
    count = rows_ref.shape[0]
    quarter = count // 4
    _, shard_rows, _ = given_ref.shape
    shard_len = shard_rows * LANES
    me = lax.axis_index("dp")

    def fetch(block):
        return pltpu.make_async_copy(
            grads_ref.at[:, pl.ds(block * shard_len, shard_len)], rows_ref.at[block], sems.at[block]
        )

    indices = pltpu.make_async_copy(perm_hbm, perm_ref, perm_sem)
    indices.start()
    for block in range(count):
        fetch(block).start()
    indices.wait()
    for device in range(count):
        owner_ref[perm_ref[device]] = device
    for block in range(count):
        offset = owner_ref[block] ^ me
        chip = offset >> 1
        by_way = (chip >= quarter) & (chip & 1 == 1)
        past = (chip - quarter) >> 1
        slot = jnp.where(by_way, past, jnp.where(chip < quarter, chip, quarter + past))
        fetch(block).wait()

        def put(far_ref, rest_ref):
            def into(out_ref):
                value = rows_ref[block]
                if out_ref.shape[1:] != value.shape:
                    value = value.reshape(shard_rows, LANES)
                out_ref[slot] = value

            lax.cond(by_way, lambda: into(far_ref), lambda: into(rest_ref))

        lax.cond(
            offset & 1 == 1,
            lambda: put(given_far_ref, given_ref),
            lambda: put(kept_far_ref, kept_ref),
        )


def fetch_blocks(grads, perm, shard_len):
    count = perm.shape[0]
    far, rest = (
        output((size, shard_len // LANES, LANES), grads.dtype)
        for size in (count // 8, count // 2 - count // 8)
    )
    raw = output((count // 2 - count // 8, 1, shard_len), grads.dtype)
    outs = pl.pallas_call(
        fetch_kernel,
        out_shape=(far, rest, far, raw),
        in_specs=[ANY, ANY],
        out_specs=(VMEM,) * 4,
        scratch_shapes=[
            pltpu.VMEM((count, 1, shard_len), grads.dtype),
            pltpu.SMEM(perm.shape, perm.dtype),
            pltpu.SMEM(perm.shape, perm.dtype),
            pltpu.SemaphoreType.DMA,
            pltpu.SemaphoreType.DMA((count,)),
        ],
        name="fetch_blocks",
    )(perm, grads)
    return outs[:2], outs[2:]


def layout_kernel(raw_ref, out_ref):
    for k in range(out_ref.shape[0]):
        out_ref[k] = raw_ref[k].reshape(out_ref.shape[1:])


def layout_blocks(raw):
    count, _, shard_len = raw.shape
    return pl.pallas_call(
        layout_kernel,
        out_shape=output((count, shard_len // LANES, LANES), raw.dtype),
        in_specs=[VMEM],
        out_specs=VMEM,
        name="layout_blocks",
    )(near(raw) if fits(1, raw.shape, raw.dtype) else raw)


def members_kernel(perm_ref, bounds_ref, master_ref, rows_ref, columns_ref, weight_ref):
    tensors = bounds_ref.shape[0] - 1
    shard_rows = master_ref.shape[0]
    me = lax.axis_index("dp")
    half = lax.axis_size("dp") // 2

    def one_hot(shape, tensor_dim, device):
        first = perm_ref[device] * shard_rows
        tensor = lax.broadcasted_iota(jnp.int32, shape, tensor_dim)
        row = lax.broadcasted_iota(jnp.int32, shape, 1 - tensor_dim)
        low = jnp.zeros(shape, jnp.int32)
        high = jnp.zeros(shape, jnp.int32)
        for t in range(tensors):
            low = jnp.where(tensor == t, bounds_ref[t] // LANES - first, low)
            high = jnp.where(tensor == t, bounds_ref[t + 1] // LANES - first, high)
        return ((row >= low) & (row < high)).astype(jnp.float32)

    rows_ref[0] = one_hot((shard_rows, tensors), 1, me)
    rows_ref[1] = one_hot((shard_rows, tensors), 1, me ^ half)
    columns = one_hot((tensors, shard_rows), 0, me)
    columns_ref[...] = columns
    weight_ref[...] = square_sums(columns, master_ref[...])


def exact_dot(left, right):
    return jnp.dot(
        left, right, precision=lax.Precision.HIGHEST, preferred_element_type=jnp.float32
    )


def square_sums(columns, value):
    return jnp.sum(exact_dot(columns, value * value), axis=1, keepdims=True)


def find_members(perm, bounds, master):
    tensors = bounds.shape[0] - 1
    shard_rows = master.shape[0]
    return pl.pallas_call(
        members_kernel,
        out_shape=(
            output((2, shard_rows, tensors), jnp.float32),
            output((tensors, shard_rows), jnp.float32),
            output((tensors, 1), jnp.float32),
        ),
        in_specs=[SMEM, SMEM, VMEM],
        out_specs=(VMEM, VMEM, VMEM),
        name="find_members",
    )(perm, bounds, near(master))


def sums_kernel(columns_ref, weight_ref, direction_ref, out_ref):
    update_sq = square_sums(columns_ref[...], direction_ref[...])
    lane = lax.broadcasted_iota(jnp.int32, out_ref.shape, 1)
    out_ref[...] = jnp.where(lane == 0, weight_ref[...], jnp.where(lane == 1, update_sq, 0.0))


def tensor_sums(columns, weight_sq, direction):
    return pl.pallas_call(
        sums_kernel,
        out_shape=output((columns.shape[0], LANES), jnp.float32),
        in_specs=[VMEM, VMEM, VMEM],
        out_specs=VMEM,
        name="tensor_sums",
    )(near(columns), near(weight_sq), near(direction))


def finish_kernel(
    rows_ref, sums_ref, masters_refs, directions_refs, step_ref, new_ref, weights_ref
):
    norms = jnp.sqrt(sums_ref[...])
    ratios = norms[:, 0:1] / (norms[:, 1:2] + norm_eps)
    ratios = jnp.broadcast_to(ratios, norms.shape)
    for k in range(2):
        step = exact_dot(rows_ref[k], ratios) * directions_refs[k][...]
        new = masters_refs[k][...] - learn_rate * step
        weights_ref[k] = new.astype(jnp.bfloat16)
        if k == 0:
            step_ref[...] = step
            new_ref[...] = new


def finish(rows, sums, masters, directions):
    like = output(masters[0].shape, jnp.float32)
    weights = output((2, *masters[0].shape), jnp.bfloat16)
    return pl.pallas_call(
        finish_kernel,
        out_shape=(like, like, weights),
        in_specs=[VMEM, VMEM, (VMEM, VMEM), (VMEM, VMEM)],
        out_specs=(VMEM, VMEM, VMEM),
        name="finish",
    )(near(rows), near(sums), tuple(map(near, masters)), tuple(map(near, directions)))


def block_of(perm, device):
    lane = lax.broadcasted_iota(jnp.int32, perm.shape, 1)
    return jnp.sum(jnp.where(lane == device, perm, 0.0)).astype(jnp.int32)


def place_kernel(offsets, extra, perm_ref, *refs):
    count = len(offsets)
    sems = refs[-1]
    pieces, kept = refs[:count], refs[count : count + extra]
    out_ref, rows_out = refs[-2 - extra], refs[-1 - extra : -1]
    me = lax.axis_index("dp")
    copies = [
        pltpu.make_async_copy(source, target, sems.at[k])
        for k, (source, target) in enumerate(zip(kept, rows_out))
    ]
    for copy in copies:
        copy.start()
    perm = perm_ref[...]
    half = perm.shape[1] // 2
    for k, offset in enumerate((*offsets, *(offset ^ half for offset in offsets))):
        source = pieces[k % count].at[k // count]
        block = block_of(perm, me ^ offset)
        copies.append(pltpu.make_async_copy(source, out_ref.at[block], sems.at[extra + k]))
        copies[-1].start()
    for copy in copies:
        copy.wait()


def place(perm, pieces, rows, into=None):
    offsets = tuple(pieces)
    pieces = tuple(pieces.values())
    count = len(pieces)
    like = pieces[0]
    close = fits(count, like.shape, like.dtype)
    operands = (perm, *(map(near, pieces) if close else pieces), *map(near, rows))
    in_specs = [VMEM] + [VMEM if close else ANY] * count + [VMEM] * len(rows)
    aliases = {}
    if into is not None:
        aliases = {len(operands): 0}
        operands += (into,)
        in_specs.append(ANY)
    return pl.pallas_call(
        functools.partial(place_kernel, offsets, len(rows)),
        out_shape=(
            jax.ShapeDtypeStruct((perm.shape[1], *like.shape[1:]), like.dtype),
            *(jax.ShapeDtypeStruct(row.shape, row.dtype) for row in rows),
        ),
        in_specs=in_specs,
        out_specs=(ANY,) * (1 + len(rows)),
        scratch_shapes=[pltpu.SemaphoreType.DMA((2 * count + len(rows),))],
        input_output_aliases=aliases,
        name="place",
    )(*operands)


def offset_groups(high):
    groups = []
    while high > 2:
        low = max(high // 4, 2)
        hops = [k * low for k in range(1, high // low)]
        groups.append(hops)
        high = low
    return groups


def sum_groups(high):
    groups = []
    low = 2
    while low < high:
        end = min(low * 4, high)
        groups.append([k * low for k in range(end // low - 1, 0, -1)])
        low = end
    return groups


def gather_plan(count):
    known = [0]
    stages = []
    for group in offset_groups(count // 2) + [[1]]:
        stages.append([(piece, hop) for hop in group for piece in known])
        known += sorted(piece ^ hop for piece, hop in stages[-1])
    order = []
    for piece in known:
        for stage in stages:
            order += [exchange for exchange in stage if exchange[0] == piece]
    return order


def reduce_plan(half):
    far = range(half // 2, half)
    by_way = [k for k in far if k % 2]
    onward = [k for k in far if k % 2 == 0]
    return by_way, [*range(2, half // 2), *onward, 1]


def per_device(grads, master, first_moment, second_moment, perm, bounds):
    count = lax.axis_size("dp")
    if count < 8 or count & (count - 1):
        raise ValueError("unsupported dp size")
    half = count // 2
    shard_len = master.shape[1]
    shard_rows = shard_len // LANES

    def swap(value, offset):
        return lax.ppermute(value, "dp", [(i, i ^ offset) for i in range(count)])

    master = master.reshape(shard_rows, LANES)
    first_moment = first_moment.reshape(shard_rows, LANES)
    second_moment = second_moment.reshape(shard_rows, LANES)

    perm_row = near(perm.astype(jnp.float32)[None])

    given, kept = fetch_blocks(grads, perm, shard_len)
    by_way, straight = reduce_plan(half)
    groups = (by_way, [k for k in range(half) if k not in by_way])
    kept = (kept[0], layout_blocks(kept[1]))
    taken = [swap(value, 1) for value in given]
    far_master = swap(master, half)
    rows, columns, weight_sq = find_members(perm, bounds, master)

    def wire(value):
        return (value * WIRE_SCALE).astype(jnp.float16)

    def unwire(value):
        return value.astype(jnp.float32) * (1.0 / WIRE_SCALE)

    def pair_sums(index):
        return {
            k: kept[index][slot].astype(jnp.float32) + taken[index][slot].astype(jnp.float32)
            for slot, k in enumerate(groups[index])
        }

    leaving = [wire(value) for value in pair_sums(0).values()]
    added = {k ^ 1: swap(value, 2) for k, value in zip(by_way, leaving)}
    taken[1], _ = lax.optimization_barrier((taken[1], leaving[-1]))
    pairs = pair_sums(1)
    for k, value in added.items():
        pairs[k] = pairs[k] + unwire(value)
    total = pairs[0]
    arrived = [swap(wire(pairs[k]), 2 * k) for k in straight]
    for piece in arrived:
        total = total + unwire(piece)
    own_grad = total / count

    new_first = beta_first * first_moment + (1.0 - beta_first) * own_grad
    new_second = beta_second * second_moment + (1.0 - beta_second) * own_grad * own_grad
    direction = (
        new_first / first_fix / (jnp.sqrt(new_second / second_fix) + adam_eps) + decay_rate * master
    )
    sums = tensor_sums(columns, weight_sq, direction)
    sums = sums + swap(sums, half)
    far_direction = swap(direction, half)
    sums = sums + swap(sums, 1)
    for group in sum_groups(half):
        parts = [sums] + [swap(sums, hop) for hop in group][::-1]
        while len(parts) > 1:
            parts = [low + high for low, high in zip(parts[::2], parts[1::2])]
        (sums,) = parts
    step_taken, new_master, weights = finish(
        rows, sums, (master, far_master), (direction, far_direction)
    )

    pieces = {0: weights}
    for piece, hop in gather_plan(count):
        pieces[piece ^ hop] = swap(pieces[piece], hop)
    last = [k for k in sorted(pieces) if k % 2][len(pieces) // 4 :]
    new_weights, step_taken, new_master, new_first, new_second = place(
        perm_row,
        {k: piece for k, piece in pieces.items() if k not in last},
        (step_taken, new_master, new_first, new_second),
    )
    (new_weights,) = place(perm_row, {k: pieces[k] for k in last}, (), new_weights)

    def row(value):
        return value.reshape(1, shard_len)

    return (
        new_weights.reshape(-1),
        row(new_master),
        row(new_first),
        row(new_second),
        row(step_taken),
    )


def solution(mesh):
    rows = P(("section", "dp"), None)

    return jax.shard_map(
        per_device,
        mesh=mesh,
        in_specs=(rows, rows, rows, rows, P("section"), P("section")),
        out_specs=(P("section"), rows, rows, rows, rows),
        check_vma=False,
    )
```
